128 devices in a mesh: expert: 8 (over x, core), dp: 16 (over z, y).
Axes of the slice: x: 4, y: 4, z: 4, core: 2. Of those that a mesh axis runs over, the one named last changes fastest.
Arguments:
- cotangents: bfloat16 [16384, 2048], P(('expert', 'dp')), may hold values from -0.59765625 to 0.59765625
- routes: int32 [16384, 2], P(('expert', 'dp')), may hold values from 0 to 7, all different within a row; in each aligned block of 128 rows (0 to 127, 128 to 255, ...) at most 40 rows name the same one
- gate_probs: float32 [16384, 2], P(('expert', 'dp')), may hold values from 0.1 to 0.9
- hidden_now: bfloat16 [8, 16, 8, 40, 7168], P('expert', 'dp'), may hold values from -6 to 6
- hidden_prev: bfloat16 [8, 16, 8, 40, 7168], P('expert', 'dp'), may hold values from -6 to 6
- cotan_prev: bfloat16 [8, 16, 320, 2048], P('expert', 'dp'), may hold values from -0.29882812 to 0.29882812
- trigger: int32 [8, 16, 56], P('expert', 'dp'), may hold values from 0 to 1, as said below
- stale_sum: float32 [8, 7168, 2048], P('expert', None, 'dp'), may hold values from -12 to 12
Outputs:
- new_sum: float32 [8, 7168, 2048], P('expert', None, 'dp')
- margins: float32 [8, 16, 56], P('expert', 'dp')
The draws below stay inside these ranges and needn't reach their ends.
Inputs may be any that keep to these rules, and one draw needn't show every extreme that they name: `routes`: in the rows of one device each expert is named at most 40 times. `trigger`: each worker's row of 56 entries holds between 1 and 16 ones, and some worker's row holds exactly 16.
All inputs are finite; a program needn't handle non-finite values.
Results may differ from the reference program's by a relative error of at most 0.0055.
Values may be sent and summed in bfloat16 or wider, within the bound.
No kernel may reach another device: no remote copies, remote signals or barrier semaphores. Data moves between devices by JAX's collectives and lax.ppermute only.
A program may use at most 192 MiB of HBM per device.

```python
import math
import jax
import jax.numpy as jnp
import numpy as np
from jax import lax

TOK_DEV = 128
DW = 2048
FFW = 7168
BLOCK = 128
TRIG = 16
EXPERTS = 8
CAP = 40
BLOCKS = 56
TOKENS = 16384
N_DP = 16


def draw_trigger(key, part):
    workers = EXPERTS * N_DP
    count_key, pick_key, order_key = jax.random.split(key, 3)
    counts = jax.random.randint(count_key, (workers,), 1, TRIG + 1)
    busiest = jax.random.randint(pick_key, (), 0, workers)
    counts = jnp.where(jnp.arange(workers) == busiest, TRIG, counts)
    orders = jax.vmap(lambda one_key: jax.random.permutation(one_key, BLOCKS))(jax.random.split(order_key, workers))
    block_ranks = jnp.argsort(orders, axis=1)
    return (block_ranks < counts[:, None]).astype(jnp.int32).reshape(EXPERTS, N_DP, BLOCKS)


def block_scale(stream_key, dims, shards, smallest, largest):
    def one(dim, parts):
        draws = jax.random.uniform(jax.random.fold_in(jax.random.fold_in(stream_key, 6), dim), (parts,), jnp.float32, smallest / len(shards), largest / len(shards))
        return jnp.repeat(jnp.exp(draws), dims[dim] // parts).reshape((-1,) + (1,) * (len(dims) - dim - 1))

    factor_of = one(*shards[0])
    for cut in shards[1:]:
        factor_of = factor_of * one(*cut)
    return factor_of


def assign_block(own_key, own, number, rows, count, top, most, slope):
    ranking = jax.random.permutation(own_key, count)
    crowded, usual = shares(count, rows * top, most, slope, True), shares(count, rows * top, most, slope, False)
    places = jnp.arange(count)

    def named(tallies, offset_by):
        used = int((tallies > 0).sum())
        fixed = max(1, used // 4)
        moved = fixed + (places - fixed + offset_by * (used - fixed)) % max(1, count - fixed)
        return jnp.zeros((count,), jnp.int32).at[ranking[jnp.where(places < fixed, places, moved)]].set(jnp.asarray(tallies, jnp.int32))

    tallies = jnp.where(number % 4 == 0, named(crowded, number // 4), named(usual, number - number // 4 - 1))
    mixed = jax.random.permutation(jax.random.fold_in(own, 3), count)
    source_of, sink = mixed[0:count // 2 * 2:2], mixed[1:count // 2 * 2:2]
    room = jnp.minimum(tallies[source_of] - 1, most - tallies[sink]) // 2
    room = jnp.where((source_of == ranking[0]) | (sink == ranking[0]) | (tallies[sink] == 0), 0, jnp.maximum(room, 0))
    moved = jax.random.randint(jax.random.fold_in(own, 4), (count // 2,), 0, 1 << 20) % (room + 1)
    tallies = tallies.at[source_of].add(-moved).at[sink].add(moved)
    members = jnp.searchsorted(jnp.cumsum(tallies), jnp.arange(rows * top), side="right").astype(jnp.int32)
    table = members.reshape(top, rows).T
    table = table[jax.random.permutation(jax.random.fold_in(own, 1), rows)]
    offset_by = jax.random.randint(jax.random.fold_in(own, 2), (rows, 1), 0, top)
    return jnp.take_along_axis(table, (jnp.arange(top)[None, :] + offset_by) % top, axis=1)


def shares(number_of, total, most, skew, full):
    portions = [(1 << 20) // math.isqrt(standing ** skew) + 1 for standing in range(1, number_of + 1)]
    largest = most if full else min(most, max(-(-total // number_of), total * portions[0] // sum(portions)))
    least = 1 if total - largest >= number_of - 1 else 0
    given, rest = [largest] + [least] * (number_of - 1), total - largest - least * (number_of - 1)
    while rest > 0:
        candidates = [i for i in range(1, number_of) if given[i] < largest] or [i for i in range(1, number_of) if given[i] < most]
        pool, left = sum([portions[i] for i in candidates]), rest
        for i in candidates:
            more = min(most - given[i], max(1, left * portions[i] // pool), rest)
            given[i] = given[i] + more
            rest = rest - more
    return np.array(given)


def scatter_about(own_key, extent, spread, bound, cuts=(), kind=jnp.bfloat16):
    result = spread * jax.random.normal(own_key, extent, jnp.float32)
    if cuts:
        result = result * block_scale(own_key, extent, cuts, -0.22, 0.18)
    return jnp.clip(result, -bound, bound).astype(kind)


def setup_inputs(seed: int = 0) -> dict:
    key_list = jax.random.split(jax.random.key(seed), 9)
    cotangents = scatter_about(key_list[0], (TOKENS, DW), 0.1, 0.59765625, ((0, 128),))
    routes_keys = jax.random.split(jax.random.fold_in(key_list[1], 1), TOKENS // TOK_DEV)
    routes_turns = jax.random.permutation(jax.random.fold_in(key_list[1], 3), TOKENS // TOK_DEV)
    routes = jax.vmap(lambda own, number: assign_block(jax.random.fold_in(key_list[1], 2), own, number, TOK_DEV, EXPERTS, 2, CAP, 2))(routes_keys, routes_turns).reshape((TOKENS, 2))
    gate_probs = jnp.clip(0.1 + 0.79999997 * jax.random.uniform(key_list[2], (TOKENS, 2), jnp.float32) ** block_scale(key_list[2], (TOKENS, 2), ((0, 128),), -0.2, 0.2), 0.1, 0.9)
    hidden_now = scatter_about(key_list[3], (EXPERTS, N_DP, EXPERTS, CAP, FFW), 1.0, 6.0, ((0, 8), (1, 16)))
    hidden_prev = scatter_about(key_list[4], (EXPERTS, N_DP, EXPERTS, CAP, FFW), 1.0, 6.0, ((0, 8), (1, 16)))
    cotan_prev = scatter_about(key_list[5], (EXPERTS, N_DP, EXPERTS * CAP, DW), 0.05, 0.29882812, ((0, 8), (1, 16)))
    trigger = draw_trigger(jax.random.fold_in(key_list[8], 71), 0)
    stale_sum = scatter_about(key_list[7], (EXPERTS, FFW, DW), 2.0, 12.0, ((0, 8), (2, 16)), jnp.float32)
    return dict(cotangents=cotangents, routes=routes, gate_probs=gate_probs, hidden_now=hidden_now, hidden_prev=hidden_prev, cotan_prev=cotan_prev, trigger=trigger, stale_sum=stale_sum)


trigger_weight = 0.1


def slot_rows(routes_dev, probs_dev, cotan_dev):
    flat_routes = routes_dev.reshape(-1).astype(jnp.int32)
    onehot = (flat_routes[:, None] == jnp.arange(EXPERTS, dtype=jnp.int32)[None, :]).astype(jnp.int32)
    slot_ranks = jnp.sum((jnp.cumsum(onehot, axis=0) - 1) * onehot, axis=1)
    target = (flat_routes * CAP + slot_ranks).astype(jnp.int32)
    weighted = jnp.repeat(cotan_dev.astype(jnp.float32), 2, axis=0) * probs_dev.reshape(-1)[:, None]
    send_table = jnp.zeros((EXPERTS * CAP, DW), jnp.float32).at[target].add(weighted)
    return send_table.astype(jnp.bfloat16).reshape(EXPERTS, CAP, DW)


def reference(cotangents, routes, gate_probs, hidden_now, hidden_prev, cotan_prev, trigger, stale_sum):
    devices_all = EXPERTS * N_DP
    slot_tables = jax.vmap(slot_rows)(routes.reshape(devices_all, TOK_DEV, 2), gate_probs.reshape(devices_all, TOK_DEV, 2), cotangents.reshape(devices_all, TOK_DEV, DW))
    slot_tables = slot_tables.reshape(EXPERTS, N_DP, EXPERTS, CAP, DW)

    def one_expert(expert):
        def one_worker(running_sum, worker):
            arrived = slot_tables[:, worker, expert]
            stacked_left = jnp.concatenate([hidden_now[expert, worker].reshape(-1, FFW), hidden_prev[expert, worker].reshape(-1, FFW)], axis=0).astype(jnp.float32)
            stacked_right = jnp.concatenate([arrived.reshape(-1, DW), -cotan_prev[expert, worker]], axis=0).astype(jnp.float32)
            difference = jnp.dot(stacked_left.T, stacked_right, precision=lax.Precision.HIGHEST)
            blocks = difference.reshape(BLOCKS, BLOCK, DW)
            diff_norms = jnp.mean(blocks * blocks, axis=(1, 2))
            gate_values = trigger[expert, worker].astype(jnp.float32)
            sent_terms = (blocks * gate_values[:, None, None]).astype(jnp.bfloat16)
            sent_terms = lax.optimization_barrier(sent_terms).astype(jnp.float32)
            return running_sum + sent_terms, diff_norms

        zero_start = jnp.zeros((BLOCKS, BLOCK, DW), jnp.float32)
        summed_terms, diff_norms = lax.scan(one_worker, zero_start, jnp.arange(N_DP))
        new_block = stale_sum[expert] + summed_terms.reshape(FFW, DW)
        block_means = jnp.sum((new_block * new_block).reshape(BLOCKS, BLOCK * DW), axis=1) / (BLOCK * DW)
        return new_block, diff_norms - trigger_weight * block_means[None, :]

    new_sum, margins = lax.map(one_expert, jnp.arange(EXPERTS))
    return new_sum, margins
```

```python
import functools

import jax
import jax.numpy as jnp
from jax import lax
from jax.experimental import pallas as pl
from jax.experimental.pallas import tpu as pltpu
from jax.sharding import PartitionSpec as P


DW = 2048
FFW = 7168
BLOCK = 128
BLOCKS = 56
TRIG = 16
CAP = 40
LANES = 128
GROUP = 4
WIDE = 512
SIDE = 4
TAIL = 16
HALF = 8
ORDER = (1, 3, 2)
PRODUCTS_LIMITS = (44 * 1024 * 1024, 30 * 1024 * 1024)
LIMIT = 20 * 1024 * 1024
UPDATE_LIMIT = 20 * 1024 * 1024


trigger_weight = 0.1

CONTRACT_ROWS = (((0,), (0,)), ((), ()))
CONTRACT_LANES = (((1,), (1,)), ((), ()))


def plan_kernel(routes_ref, gates_ref, cotan_ref, trigger_ref, table_ref, ids_ref, ids_row_ref, trig_scr):
    tokens = cotan_ref.shape[0]
    experts = table_ref.shape[0]
    routes = routes_ref[...]
    gates = gates_ref[...]
    expert_ids = lax.broadcasted_iota(jnp.int32, (experts, tokens), 0)
    first = routes[0:1, :] == expert_ids
    second = routes[1:2, :] == expert_ids
    named = jnp.where(first | second, 1.0, 0.0)
    gate_of = jnp.where(first, gates[0:1, :], 0.0) + jnp.where(second, gates[1:2, :], 0.0)
    earlier = jnp.where(
        lax.broadcasted_iota(jnp.int32, (tokens, tokens), 0)
        < lax.broadcasted_iota(jnp.int32, (tokens, tokens), 1),
        1.0,
        0.0,
    ).astype(jnp.bfloat16)
    ranks = jnp.dot(named.astype(jnp.bfloat16), earlier, preferred_element_type=jnp.float32)
    slot_ids = lax.broadcasted_iota(jnp.int32, (CAP, tokens), 0).astype(jnp.float32)
    cotan = cotan_ref[...]
    for e in range(experts):
        pick = jnp.where((slot_ids == ranks[e : e + 1, :]) & (named[e : e + 1, :] > 0.5), 1.0, 0.0)
        gate_slot = jnp.sum(pick * gate_of[e : e + 1, :], axis=1, keepdims=True)
        rows = jnp.dot(pick.astype(jnp.bfloat16), cotan, preferred_element_type=jnp.float32)
        table_ref[e] = (rows * gate_slot).astype(jnp.bfloat16)

    trig_scr[...] = jnp.zeros_like(trig_scr)
    trig_scr[0:1, 0:BLOCKS] = trigger_ref[...].astype(jnp.float32)
    trig = trig_scr[...]
    earlier_b = jnp.where(
        lax.broadcasted_iota(jnp.int32, (LANES, LANES), 0)
        < lax.broadcasted_iota(jnp.int32, (LANES, LANES), 1),
        1.0,
        0.0,
    ).astype(jnp.bfloat16)
    block_ranks = jnp.dot(trig.astype(jnp.bfloat16), earlier_b, preferred_element_type=jnp.float32)
    rank_ids = lax.broadcasted_iota(jnp.int32, (LANES, LANES), 0).astype(jnp.float32)
    match = jnp.where((rank_ids == block_ranks[0:1, :]) & (trig[0:1, :] > 0.5), 1.0, 0.0)
    lane_ids = lax.broadcasted_iota(jnp.int32, (LANES, LANES), 1).astype(jnp.float32)
    column = jnp.sum(match * (lane_ids - 64.0), axis=1, keepdims=True) + 64.0
    ids_ref[...] = jnp.broadcast_to(column[0:TRIG], (TRIG, LANES)).astype(jnp.int32)
    offsets = (lax.broadcasted_iota(jnp.int32, (16, LANES), 1).astype(jnp.float32) - 64.0).astype(jnp.bfloat16)
    row = lax.dot_general(offsets, match.astype(jnp.bfloat16), CONTRACT_LANES, preferred_element_type=jnp.float32)
    ids_row_ref[...] = (row[0:1, :] + 64.0).astype(jnp.int32)


def plan(routes, gates, cotan, trigger, experts):
    return pl.pallas_call(
        plan_kernel,
        out_shape=(
            jax.ShapeDtypeStruct((experts, CAP, DW), jnp.bfloat16),
            jax.ShapeDtypeStruct((TRIG, LANES), jnp.int32),
            jax.ShapeDtypeStruct((1, LANES), jnp.int32),
        ),
        scratch_shapes=[pltpu.VMEM((8, LANES), jnp.float32)],
        cost_estimate=pl.CostEstimate(flops=200_000_000, bytes_accessed=2_000_000, transcendentals=0),
        name="plan",
    )(routes, gates, cotan, trigger)


def join(left_ref, at, now, prev):
    rows = now.shape[0]
    left_ref[0:rows, at] = now
    left_ref[rows:, at] = prev


def join_right(right_ref, slots_ref, cotan_ref):
    rows = slots_ref.shape[0]
    right_ref[0:rows, :] = slots_ref[...]
    right_ref[rows:, :] = -cotan_ref[...]


def products_kernel(start, count, z_first, ids_ref, place_ref, row_ref, now_hbm, prev_hbm, slots_ref, cotan_ref, *refs):
    out_refs = refs[0:SIDE]
    left_ref, right_ref, now_sems, prev_sems = refs[SIDE:]
    rows = slots_ref.shape[0]
    copies = []
    for j in range(count):
        block = lax.rem(ids_ref[start + j, 0], 64)
        come = pl.ds(pl.multiple_of(block * BLOCK, BLOCK), BLOCK)
        at = pl.ds(j * BLOCK, BLOCK)
        copies.append(pltpu.make_async_copy(now_hbm.at[:, come], left_ref.at[pl.ds(0, rows), at], now_sems.at[j]))
        copies.append(pltpu.make_async_copy(prev_hbm.at[:, come], left_ref.at[pl.ds(rows, rows), at], prev_sems.at[j]))
    for copy in copies:
        copy.start()
    for t in range(SIDE):
        for s in range(SIDE):
            server = ((place_ref[0] + t) % SIDE) * SIDE + (place_ref[1] + s) % SIDE
            come = pl.ds(pl.multiple_of(server * LANES, LANES), LANES)
            at = slice((t * SIDE + s) * LANES, (t * SIDE + s + 1) * LANES)
            right_ref[0:rows, at] = slots_ref[:, come]
            right_ref[rows:, at] = -cotan_ref[:, come]
    row = jnp.broadcast_to(row_ref[...].astype(jnp.float32), (TAIL, LANES)).astype(jnp.bfloat16)
    for out_ref in out_refs:
        for s in range(SIDE):
            out_ref[s, count * BLOCK : count * BLOCK + TAIL, :] = row
    for g in range(count // GROUP):
        for copy in copies[2 * g * GROUP : 2 * (g + 1) * GROUP]:
            copy.wait()
        at = slice(g * GROUP * BLOCK, (g + 1) * GROUP * BLOCK)
        for t in range(SIDE):
            acc = lax.dot_general(
                left_ref[:, at],
                right_ref[:, t * SIDE * LANES : (t + 1) * SIDE * LANES],
                CONTRACT_ROWS,
                preferred_element_type=jnp.float32,
            )
            for s in range(SIDE):
                piece = acc[:, s * LANES : (s + 1) * LANES].astype(jnp.bfloat16)
                if z_first:
                    out_refs[t][s, at, :] = piece
                else:
                    out_refs[s][t, at, :] = piece


def products(ids, place, row, now, prev, slots, cotan, start, count, z_first):
    rows = now.shape[0]
    vmem = pl.BlockSpec(memory_space=pltpu.VMEM)
    smem = pl.BlockSpec(memory_space=pltpu.SMEM)
    hbm = pl.BlockSpec(memory_space=pltpu.HBM)
    return pl.pallas_call(
        functools.partial(products_kernel, start, count, z_first),
        out_shape=[jax.ShapeDtypeStruct((SIDE, count * BLOCK + TAIL, LANES), jnp.bfloat16)] * SIDE,
        in_specs=[smem, smem, vmem, hbm, hbm, vmem, vmem],
        out_specs=[vmem] * SIDE,
        scratch_shapes=[
            pltpu.VMEM((2 * rows, count * BLOCK), jnp.bfloat16),
            pltpu.VMEM((2 * rows, DW), jnp.bfloat16),
            pltpu.SemaphoreType.DMA((count,)),
            pltpu.SemaphoreType.DMA((count,)),
        ],
        compiler_params=pltpu.CompilerParams(vmem_limit_bytes=PRODUCTS_LIMITS[z_first]),
        cost_estimate=pl.CostEstimate(
            flops=4 * rows * BLOCK * DW * count, bytes_accessed=count * 700_000 + 2_600_000, transcendentals=0
        ),
        name="products",
    )(ids, place, row, now, prev, slots, cotan)


def norms_kernel(now_ref, prev_ref, slots_ref, cotan_ref, out_ref, left_ref, right_ref):
    @pl.when(pl.program_id(0) == 0)
    def _():
        join_right(right_ref, slots_ref, cotan_ref)

    join(left_ref, slice(None), now_ref[...], prev_ref[...])
    totals = [jnp.zeros((1, LANES), jnp.float32)] * GROUP
    for n in range(DW // WIDE):
        acc = lax.dot_general(
            left_ref[...],
            right_ref[:, n * WIDE : (n + 1) * WIDE],
            CONTRACT_ROWS,
            preferred_element_type=jnp.float32,
        )
        for j in range(GROUP):
            part = acc[j * BLOCK : (j + 1) * BLOCK, :]
            sums = jnp.sum(part * part, axis=0, keepdims=True)
            for s in range(WIDE // LANES):
                totals[j] = totals[j] + sums[:, s * LANES : (s + 1) * LANES]
    for j in range(GROUP):
        out_ref[j] = totals[j]


def norms(now, prev, slots, cotan):
    rows = now.shape[0]
    return pl.pallas_call(
        norms_kernel,
        out_shape=jax.ShapeDtypeStruct((BLOCKS, 1, LANES), jnp.float32),
        grid=(BLOCKS // GROUP,),
        in_specs=[
            pl.BlockSpec((rows, GROUP * BLOCK), lambda b: (0, b)),
            pl.BlockSpec((rows, GROUP * BLOCK), lambda b: (0, b)),
            pl.BlockSpec((rows, DW), lambda b: (0, 0)),
            pl.BlockSpec((rows, DW), lambda b: (0, 0)),
        ],
        out_specs=pl.BlockSpec((GROUP, 1, LANES), lambda b: (b, 0, 0)),
        scratch_shapes=[
            pltpu.VMEM((2 * rows, GROUP * BLOCK), jnp.bfloat16),
            pltpu.VMEM((2 * rows, DW), jnp.bfloat16),
        ],
        compiler_params=pltpu.CompilerParams(dimension_semantics=("arbitrary",), vmem_limit_bytes=LIMIT),
        cost_estimate=pl.CostEstimate(
            flops=4 * rows * FFW * DW, bytes_accessed=4 * rows * FFW + 2_600_000, transcendentals=0
        ),
        name="norms",
    )(now, prev, slots, cotan)


def update_kernel(pieces, last, base_ref, *refs):
    got_refs, (out_ref, *rest) = refs[: len(pieces)], refs[len(pieces) :]
    ids_scr, ids_ref, ids_sem = rest[-3:]
    row = 0
    for got_ref, (parts, _) in zip(got_refs, pieces):
        for k in range(parts):
            tail = got_ref[k, got_ref.shape[1] - TAIL :, :].astype(jnp.float32)
            ids_scr[row : row + 1, :] = tail[0:1, :].astype(jnp.int32)
            row += 1
    copy = pltpu.make_async_copy(ids_scr, ids_ref, ids_sem)
    copy.start()
    out_ref[...] = base_ref[...]
    copy.wait()
    row = 0
    for got_ref, (parts, start) in zip(got_refs, pieces):
        count = got_ref.shape[1] // BLOCK
        for k in range(parts):

            def add(j, carry, got_ref=got_ref, k=k, row=row, start=start):
                block = ids_ref[row, start + j]

                @pl.when(block < 64)
                def _():
                    at = pl.ds(pl.multiple_of(block * BLOCK, BLOCK), BLOCK)
                    come = pl.ds(pl.multiple_of(j * BLOCK, BLOCK), BLOCK)
                    out_ref[at, :] += got_ref[k, come, :].astype(jnp.float32)

                return carry

            lax.fori_loop(0, count, add, 0)
            row += 1
    if last:
        squares_ref, scr = rest[0], rest[1]
        scr[...] = jnp.zeros_like(scr)
        for b in range(BLOCKS):
            x = out_ref[b * BLOCK : (b + 1) * BLOCK, :]
            scr[b : b + 1, :] = jnp.sum(x * x, axis=0, keepdims=True)
        squares_ref[...] = lax.dot_general(
            jnp.ones((16, LANES), jnp.float32),
            scr[...],
            CONTRACT_LANES,
            precision=lax.Precision.HIGHEST,
            preferred_element_type=jnp.float32,
        )


def update(base, got, pieces, last):
    vmem = pl.BlockSpec(memory_space=pltpu.VMEM)
    out_shape = [jax.ShapeDtypeStruct(base.shape, jnp.float32)]
    scratch = []
    if last:
        out_shape.append(jax.ShapeDtypeStruct((16, LANES), jnp.float32))
        scratch.append(pltpu.VMEM((LANES, LANES), jnp.float32))
    rows = -(-sum(parts for parts, _ in pieces) // 8) * 8
    return pl.pallas_call(
        functools.partial(update_kernel, pieces, last),
        out_shape=out_shape,
        in_specs=[vmem] * (1 + len(got)),
        out_specs=[vmem] * len(out_shape),
        scratch_shapes=[
            *scratch,
            pltpu.VMEM((rows, LANES), jnp.int32),
            pltpu.SMEM((rows, LANES), jnp.int32),
            pltpu.SemaphoreType.DMA,
        ],
        compiler_params=pltpu.CompilerParams(vmem_limit_bytes=UPDATE_LIMIT),
        cost_estimate=pl.CostEstimate(flops=5_000_000_000, bytes_accessed=16_000_000, transcendentals=0),
        name="update_last" if last else "update",
    )(base, *got)


def shift(workers, dz, dy):
    side = SIDE
    return [
        (z * side + y, ((z + dz) % side) * side + (y + dy) % side) for z in range(workers // side) for y in range(side)
    ]


def local(cotangents, routes, gate_probs, hidden_now, hidden_prev, cotan_prev, trigger, stale_sum):
    experts = lax.axis_size("expert")
    workers = lax.axis_size("dp")
    columns = DW // workers
    table, ids, ids_row = plan(routes.T, gate_probs.T, cotangents, trigger.reshape(1, BLOCKS), experts)
    exchange = functools.partial(lax.all_to_all, split_axis=0, concat_axis=0, tiled=True)
    slots = exchange(table, "expert").reshape(-1, DW)
    now = hidden_now.reshape(-1, FFW)
    prev = hidden_prev.reshape(-1, FFW)
    cotan = cotan_prev.reshape(-1, DW)
    here = lax.axis_index("dp")
    place = jnp.stack([here // SIDE, here % SIDE]).astype(jnp.int32)

    def along_y(x, k):
        return lax.ppermute(x, "dp", shift(workers, 0, k))

    def along_z(x, k):
        return lax.ppermute(x, "dp", shift(workers, k, 0))

    sent_a = products(ids, place, ids_row, now, prev, slots, cotan, 0, HALF, False)
    first_a, first_b = {0: sent_a[0]}, {}
    for k in ORDER:
        first_a[k] = along_y(sent_a[k], k)
    sent_b = products(ids, place, ids_row, now, prev, slots, cotan, HALF, HALF, True)
    first_b[0] = sent_b[0]
    for k in ORDER:
        first_b[k] = along_z(sent_b[k], k)
    squared = norms(now, prev, slots, cotan)
    first_a, squared = lax.optimization_barrier((first_a, squared))
    second_a, second_b = {}, {}
    for k in ORDER:
        second_a[k] = along_z(jnp.stack([first_a[j][k] for j in range(SIDE)]), k)
    for k in ORDER:
        second_b[k] = along_y(jnp.stack([first_b[j][k] for j in range(SIDE)]), k)
    diff_norms = jnp.sum(squared, axis=(1, 2)) / (BLOCK * DW)
    (current,) = update(
        stale_sum.reshape(FFW, columns),
        [first_a[k] for k in range(SIDE)] + [first_b[k] for k in range(SIDE)],
        [(1, 0)] * SIDE + [(1, HALF)] * SIDE,
        False,
    )
    (current,) = update(
        current,
        [second_a[k] for k in ORDER[:2]] + [second_b[k] for k in ORDER[:2]],
        [(SIDE, 0)] * 2 + [(SIDE, HALF)] * 2,
        False,
    )
    current, squares = update(
        current, [second_a[ORDER[2]], second_b[ORDER[2]]], [(SIDE, 0), (SIDE, HALF)], True
    )
    everyone = exchange(squares.reshape(workers, 1, LANES), "dp").reshape(workers, LANES)
    norm_totals = jnp.sum(everyone, axis=0)[:BLOCKS] / (BLOCK * DW)
    margins = diff_norms - trigger_weight * norm_totals
    return (current.reshape(1, FFW, columns), margins.reshape(1, 1, BLOCKS))


def solution(mesh):
    return jax.shard_map(
        local,
        mesh=mesh,
        in_specs=(
            P(("expert", "dp"), None),
            P(("expert", "dp"), None),
            P(("expert", "dp"), None),
            P("expert", "dp", None, None, None),
            P("expert", "dp", None, None, None),
            P("expert", "dp", None, None),
            P("expert", "dp", None),
            P("expert", None, "dp"),
        ),
        out_specs=(P("expert", None, "dp"), P("expert", "dp", None)),
        check_vma=False,
    )
```

```python
import functools

import jax
import jax.numpy as jnp
from jax import lax
from jax.experimental import pallas as pl
from jax.experimental.pallas import tpu as pltpu
from jax.sharding import PartitionSpec as P


DW = 2048
FFW = 7168
BLOCK = 128
BLOCKS = 56
TRIG = 16
CAP = 40
LANES = 128
GROUP = 4
WIDE = 512
SIDE = 4
TAIL = 16
HALF = 8
ORDER = (1, 3, 2)
PRODUCTS_LIMITS = (44 * 1024 * 1024, 30 * 1024 * 1024)
LIMIT = 20 * 1024 * 1024
UPDATE_LIMIT = 20 * 1024 * 1024


trigger_weight = 0.1

CONTRACT_ROWS = (((0,), (0,)), ((), ()))
CONTRACT_LANES = (((1,), (1,)), ((), ()))


def plan_kernel(routes_ref, gates_ref, cotan_ref, trigger_ref, table_ref, ids_ref, ids_row_ref, trig_scr):
    tokens = cotan_ref.shape[0]
    experts = table_ref.shape[0]
    routes = routes_ref[...]
    gates = gates_ref[...]
    expert_ids = lax.broadcasted_iota(jnp.int32, (experts, tokens), 0)
    first = routes[0:1, :] == expert_ids
    second = routes[1:2, :] == expert_ids
    named = jnp.where(first | second, 1.0, 0.0)
    gate_of = jnp.where(first, gates[0:1, :], 0.0) + jnp.where(second, gates[1:2, :], 0.0)
    earlier = jnp.where(
        lax.broadcasted_iota(jnp.int32, (tokens, tokens), 0)
        < lax.broadcasted_iota(jnp.int32, (tokens, tokens), 1),
        1.0,
        0.0,
    ).astype(jnp.bfloat16)
    ranks = jnp.dot(named.astype(jnp.bfloat16), earlier, preferred_element_type=jnp.float32)
    slot_ids = lax.broadcasted_iota(jnp.int32, (CAP, tokens), 0).astype(jnp.float32)
    cotan = cotan_ref[...]
    for e in range(experts):
        pick = jnp.where((slot_ids == ranks[e : e + 1, :]) & (named[e : e + 1, :] > 0.5), 1.0, 0.0)
        gate_slot = jnp.sum(pick * gate_of[e : e + 1, :], axis=1, keepdims=True)
        rows = jnp.dot(pick.astype(jnp.bfloat16), cotan, preferred_element_type=jnp.float32)
        table_ref[e] = (rows * gate_slot).astype(jnp.bfloat16)

    trig_scr[...] = jnp.zeros_like(trig_scr)
    trig_scr[0:1, 0:BLOCKS] = trigger_ref[...].astype(jnp.float32)
    trig = trig_scr[...]
    earlier_b = jnp.where(
        lax.broadcasted_iota(jnp.int32, (LANES, LANES), 0)
        < lax.broadcasted_iota(jnp.int32, (LANES, LANES), 1),
        1.0,
        0.0,
    ).astype(jnp.bfloat16)
    block_ranks = jnp.dot(trig.astype(jnp.bfloat16), earlier_b, preferred_element_type=jnp.float32)
    rank_ids = lax.broadcasted_iota(jnp.int32, (LANES, LANES), 0).astype(jnp.float32)
    match = jnp.where((rank_ids == block_ranks[0:1, :]) & (trig[0:1, :] > 0.5), 1.0, 0.0)
    lane_ids = lax.broadcasted_iota(jnp.int32, (LANES, LANES), 1).astype(jnp.float32)
    column = jnp.sum(match * (lane_ids - 64.0), axis=1, keepdims=True) + 64.0
    ids_ref[...] = jnp.broadcast_to(column[0:TRIG], (TRIG, LANES)).astype(jnp.int32)
    offsets = (lax.broadcasted_iota(jnp.int32, (16, LANES), 1).astype(jnp.float32) - 64.0).astype(jnp.bfloat16)
    row = lax.dot_general(offsets, match.astype(jnp.bfloat16), CONTRACT_LANES, preferred_element_type=jnp.float32)
    ids_row_ref[...] = (row[0:1, :] + 64.0).astype(jnp.int32)


def plan(routes, gates, cotan, trigger, experts):
    return pl.pallas_call(
        plan_kernel,
        out_shape=(
            jax.ShapeDtypeStruct((experts, CAP, DW), jnp.bfloat16),
            jax.ShapeDtypeStruct((TRIG, LANES), jnp.int32),
            jax.ShapeDtypeStruct((1, LANES), jnp.int32),
        ),
        scratch_shapes=[pltpu.VMEM((8, LANES), jnp.float32)],
        cost_estimate=pl.CostEstimate(flops=200_000_000, bytes_accessed=2_000_000, transcendentals=0),
        name="plan",
    )(routes, gates, cotan, trigger)


def join(left_ref, at, now, prev):
    rows = now.shape[0]
    left_ref[0:rows, at] = now
    left_ref[rows:, at] = prev


def join_right(right_ref, slots_ref, cotan_ref):
    rows = slots_ref.shape[0]
    right_ref[0:rows, :] = slots_ref[...]
    right_ref[rows:, :] = -cotan_ref[...]


def products_kernel(start, count, z_first, ids_ref, place_ref, row_ref, now_hbm, prev_hbm, slots_ref, cotan_ref, *refs):
    own_refs, far_refs = refs[0:SIDE], (None, *refs[SIDE : 2 * SIDE - 1])
    left_ref, right_ref, now_sems, prev_sems = refs[2 * SIDE - 1 :]
    rows = slots_ref.shape[0]
    copies = []
    for j in range(count):
        block = lax.rem(ids_ref[start + j, 0], 64)
        come = pl.ds(pl.multiple_of(block * BLOCK, BLOCK), BLOCK)
        at = pl.ds(j * BLOCK, BLOCK)
        copies.append(pltpu.make_async_copy(now_hbm.at[:, come], left_ref.at[pl.ds(0, rows), at], now_sems.at[j]))
        copies.append(pltpu.make_async_copy(prev_hbm.at[:, come], left_ref.at[pl.ds(rows, rows), at], prev_sems.at[j]))
    for copy in copies:
        copy.start()
    for t in range(SIDE):
        for s in range(SIDE):
            server = ((place_ref[0] + t) % SIDE) * SIDE + (place_ref[1] + s) % SIDE
            come = pl.ds(pl.multiple_of(server * LANES, LANES), LANES)
            at = slice((t * SIDE + s) * LANES, (t * SIDE + s + 1) * LANES)
            right_ref[0:rows, at] = slots_ref[:, come]
            right_ref[rows:, at] = -cotan_ref[:, come]
    row = jnp.broadcast_to(row_ref[...].astype(jnp.float32), (TAIL, LANES)).astype(jnp.bfloat16)
    behind = slice(count * BLOCK, count * BLOCK + TAIL)
    for k in range(SIDE):
        own_refs[k][0, behind, :] = row
        for m in range(1, SIDE):
            far_refs[m][k, behind, :] = row
    for g in range(count // GROUP):
        for copy in copies[2 * g * GROUP : 2 * (g + 1) * GROUP]:
            copy.wait()
        at = slice(g * GROUP * BLOCK, (g + 1) * GROUP * BLOCK)
        for t in range(SIDE):
            acc = lax.dot_general(
                left_ref[:, at],
                right_ref[:, t * SIDE * LANES : (t + 1) * SIDE * LANES],
                CONTRACT_ROWS,
                preferred_element_type=jnp.float32,
            )
            for s in range(SIDE):
                piece = acc[:, s * LANES : (s + 1) * LANES].astype(jnp.bfloat16)
                first, second = (t, s) if z_first else (s, t)
                if first == 0:
                    own_refs[second][0, at, :] = piece
                else:
                    far_refs[first][second, at, :] = piece


def products(ids, place, row, now, prev, slots, cotan, start, count, z_first):
    rows = now.shape[0]
    vmem = pl.BlockSpec(memory_space=pltpu.VMEM)
    smem = pl.BlockSpec(memory_space=pltpu.SMEM)
    hbm = pl.BlockSpec(memory_space=pltpu.HBM)
    return pl.pallas_call(
        functools.partial(products_kernel, start, count, z_first),
        out_shape=[jax.ShapeDtypeStruct((1, count * BLOCK + TAIL, LANES), jnp.bfloat16)] * SIDE
        + [jax.ShapeDtypeStruct((SIDE, count * BLOCK + TAIL, LANES), jnp.bfloat16)] * (SIDE - 1),
        in_specs=[smem, smem, vmem, hbm, hbm, vmem, vmem],
        out_specs=[vmem] * (2 * SIDE - 1),
        scratch_shapes=[
            pltpu.VMEM((2 * rows, count * BLOCK), jnp.bfloat16),
            pltpu.VMEM((2 * rows, DW), jnp.bfloat16),
            pltpu.SemaphoreType.DMA((count,)),
            pltpu.SemaphoreType.DMA((count,)),
        ],
        compiler_params=pltpu.CompilerParams(vmem_limit_bytes=PRODUCTS_LIMITS[z_first]),
        cost_estimate=pl.CostEstimate(
            flops=4 * rows * BLOCK * DW * count, bytes_accessed=count * 700_000 + 2_600_000, transcendentals=0
        ),
        name="products",
    )(ids, place, row, now, prev, slots, cotan)


def norms_kernel(now_ref, prev_ref, slots_ref, cotan_ref, out_ref, left_ref, right_ref):
    @pl.when(pl.program_id(0) == 0)
    def _():
        join_right(right_ref, slots_ref, cotan_ref)

    join(left_ref, slice(None), now_ref[...], prev_ref[...])
    totals = [jnp.zeros((1, LANES), jnp.float32)] * GROUP
    for n in range(DW // WIDE):
        acc = lax.dot_general(
            left_ref[...],
            right_ref[:, n * WIDE : (n + 1) * WIDE],
            CONTRACT_ROWS,
            preferred_element_type=jnp.float32,
        )
        for j in range(GROUP):
            part = acc[j * BLOCK : (j + 1) * BLOCK, :]
            sums = jnp.sum(part * part, axis=0, keepdims=True)
            for s in range(WIDE // LANES):
                totals[j] = totals[j] + sums[:, s * LANES : (s + 1) * LANES]
    for j in range(GROUP):
        out_ref[j] = totals[j]


def norms(now, prev, slots, cotan):
    rows = now.shape[0]
    return pl.pallas_call(
        norms_kernel,
        out_shape=jax.ShapeDtypeStruct((BLOCKS, 1, LANES), jnp.float32),
        grid=(BLOCKS // GROUP,),
        in_specs=[
            pl.BlockSpec((rows, GROUP * BLOCK), lambda b: (0, b)),
            pl.BlockSpec((rows, GROUP * BLOCK), lambda b: (0, b)),
            pl.BlockSpec((rows, DW), lambda b: (0, 0)),
            pl.BlockSpec((rows, DW), lambda b: (0, 0)),
        ],
        out_specs=pl.BlockSpec((GROUP, 1, LANES), lambda b: (b, 0, 0)),
        scratch_shapes=[
            pltpu.VMEM((2 * rows, GROUP * BLOCK), jnp.bfloat16),
            pltpu.VMEM((2 * rows, DW), jnp.bfloat16),
        ],
        compiler_params=pltpu.CompilerParams(dimension_semantics=("arbitrary",), vmem_limit_bytes=LIMIT),
        cost_estimate=pl.CostEstimate(
            flops=4 * rows * FFW * DW, bytes_accessed=4 * rows * FFW + 2_600_000, transcendentals=0
        ),
        name="norms",
    )(now, prev, slots, cotan)


def update_kernel(pieces, last, base_ref, *refs):
    got_refs, (out_ref, *rest) = refs[: len(pieces)], refs[len(pieces) :]
    ids_scr, ids_ref, ids_sem = rest[-3:]
    row = 0
    for got_ref, (parts, _) in zip(got_refs, pieces):
        for k in range(parts):
            tail = got_ref[k, got_ref.shape[1] - TAIL :, :].astype(jnp.float32)
            ids_scr[row : row + 1, :] = tail[0:1, :].astype(jnp.int32)
            row += 1
    copy = pltpu.make_async_copy(ids_scr, ids_ref, ids_sem)
    copy.start()
    out_ref[...] = base_ref[...]
    copy.wait()
    row = 0
    for got_ref, (parts, start) in zip(got_refs, pieces):
        count = got_ref.shape[1] // BLOCK
        for k in range(parts):

            def add(j, carry, got_ref=got_ref, k=k, row=row, start=start):
                block = ids_ref[row, start + j]

                @pl.when(block < 64)
                def _():
                    at = pl.ds(pl.multiple_of(block * BLOCK, BLOCK), BLOCK)
                    come = pl.ds(pl.multiple_of(j * BLOCK, BLOCK), BLOCK)
                    out_ref[at, :] += got_ref[k, come, :].astype(jnp.float32)

                return carry

            lax.fori_loop(0, count, add, 0)
            row += 1
    if last:
        squares_ref, scr = rest[0], rest[1]
        scr[...] = jnp.zeros_like(scr)
        for b in range(BLOCKS):
            x = out_ref[b * BLOCK : (b + 1) * BLOCK, :]
            scr[b : b + 1, :] = jnp.sum(x * x, axis=0, keepdims=True)
        squares_ref[...] = lax.dot_general(
            jnp.ones((16, LANES), jnp.float32),
            scr[...],
            CONTRACT_LANES,
            precision=lax.Precision.HIGHEST,
            preferred_element_type=jnp.float32,
        )


def update(base, got, pieces, last):
    vmem = pl.BlockSpec(memory_space=pltpu.VMEM)
    out_shape = [jax.ShapeDtypeStruct(base.shape, jnp.float32)]
    scratch = []
    if last:
        out_shape.append(jax.ShapeDtypeStruct((16, LANES), jnp.float32))
        scratch.append(pltpu.VMEM((LANES, LANES), jnp.float32))
    rows = -(-sum(parts for parts, _ in pieces) // 8) * 8
    return pl.pallas_call(
        functools.partial(update_kernel, pieces, last),
        out_shape=out_shape,
        in_specs=[vmem] * (1 + len(got)),
        out_specs=[vmem] * len(out_shape),
        scratch_shapes=[
            *scratch,
            pltpu.VMEM((rows, LANES), jnp.int32),
            pltpu.SMEM((rows, LANES), jnp.int32),
            pltpu.SemaphoreType.DMA,
        ],
        compiler_params=pltpu.CompilerParams(vmem_limit_bytes=UPDATE_LIMIT),
        cost_estimate=pl.CostEstimate(flops=5_000_000_000, bytes_accessed=16_000_000, transcendentals=0),
        name="update_last" if last else "update",
    )(base, *got)


def shift(workers, dz, dy):
    side = SIDE
    return [
        (z * side + y, ((z + dz) % side) * side + (y + dy) % side) for z in range(workers // side) for y in range(side)
    ]


def local(cotangents, routes, gate_probs, hidden_now, hidden_prev, cotan_prev, trigger, stale_sum):
    experts = lax.axis_size("expert")
    workers = lax.axis_size("dp")
    columns = DW // workers
    table, ids, ids_row = plan(routes.T, gate_probs.T, cotangents, trigger.reshape(1, BLOCKS), experts)
    exchange = functools.partial(lax.all_to_all, split_axis=0, concat_axis=0, tiled=True)
    slots = exchange(table, "expert").reshape(-1, DW)
    now = hidden_now.reshape(-1, FFW)
    prev = hidden_prev.reshape(-1, FFW)
    cotan = cotan_prev.reshape(-1, DW)
    here = lax.axis_index("dp")
    place = jnp.stack([here // SIDE, here % SIDE]).astype(jnp.int32)

    def along_y(x, k):
        return lax.ppermute(x, "dp", shift(workers, 0, k))

    def along_z(x, k):
        return lax.ppermute(x, "dp", shift(workers, k, 0))

    def stage_one(start, z_first, near, far):
        sent = products(ids, place, ids_row, now, prev, slots, cotan, start, HALF, z_first)
        own, relay = {0: sent[0]}, {}
        for k in ORDER:
            relay[k] = near(sent[SIDE - 1 + k], k)
        for k in ORDER:
            own[k] = far(sent[k], k)
        return own, relay

    def stage_two(relay, far):
        got = {}
        for k in ORDER:
            got[k] = far(jnp.stack([relay[j][k] for j in range(1, SIDE)]), k)
        return got

    own_a, relay_a = stage_one(0, False, along_y, along_z)
    own_b, relay_b = stage_one(HALF, True, along_z, along_y)
    squared = norms(now, prev, slots, cotan)
    relay_a, squared = lax.optimization_barrier((relay_a, squared))
    second_a = stage_two(relay_a, along_z)
    second_b = stage_two(relay_b, along_y)
    diff_norms = jnp.sum(squared, axis=(1, 2)) / (BLOCK * DW)
    near_a = [own_a[k] for k in range(SIDE)] + [relay_a[k] for k in ORDER]
    near_b = [own_b[k] for k in range(SIDE)] + [relay_b[k] for k in ORDER]
    (current,) = update(
        stale_sum.reshape(FFW, columns),
        near_a + near_b,
        [(1, 0)] * len(near_a) + [(1, HALF)] * len(near_b),
        False,
    )
    (current,) = update(
        current,
        [second_a[k] for k in ORDER[:2]] + [second_b[k] for k in ORDER[:2]],
        [(SIDE - 1, 0)] * 2 + [(SIDE - 1, HALF)] * 2,
        False,
    )
    current, squares = update(
        current, [second_a[ORDER[2]], second_b[ORDER[2]]], [(SIDE - 1, 0), (SIDE - 1, HALF)], True
    )
    everyone = exchange(squares.reshape(workers, 1, LANES), "dp").reshape(workers, LANES)
    norm_totals = jnp.sum(everyone, axis=0)[:BLOCKS] / (BLOCK * DW)
    margins = diff_norms - trigger_weight * norm_totals
    return (current.reshape(1, FFW, columns), margins.reshape(1, 1, BLOCKS))


def solution(mesh):
    return jax.shard_map(
        local,
        mesh=mesh,
        in_specs=(
            P(("expert", "dp"), None),
            P(("expert", "dp"), None),
            P(("expert", "dp"), None),
            P("expert", "dp", None, None, None),
            P("expert", "dp", None, None, None),
            P("expert", "dp", None, None),
            P("expert", "dp", None),
            P("expert", None, "dp"),
        ),
        out_specs=(P("expert", None, "dp"), P("expert", "dp", None)),
        check_vma=False,
    )
```

```python
import functools

import jax
import jax.numpy as jnp
from jax import lax
from jax.experimental import pallas as pl
from jax.experimental.pallas import tpu as pltpu
from jax.sharding import PartitionSpec as P


DW = 2048
FFW = 7168
BLOCK = 128
BLOCKS = 56
TRIG = 16
CAP = 40
LANES = 128
GROUP = 4
WIDE = 512
SIDE = 4
TAIL = 16
HALF = 8
ORDER = (1, 3, 2)
HOPS = (4, 5, 2, 6, 3, 7, 1)
PLAN_LIMIT = 58 * 1024 * 1024
FETCH_LIMIT = 16 * 1024 * 1024
PRODUCTS_LIMIT = 16 * 1024 * 1024
LIMIT = 20 * 1024 * 1024
UPDATE_LIMIT = 20 * 1024 * 1024


trigger_weight = 0.1

CONTRACT_ROWS = (((0,), (0,)), ((), ()))
CONTRACT_LANES = (((1,), (1,)), ((), ()))


def plan_kernel(routes_ref, gates_ref, cotan_ref, trigger_ref, *refs):
    table_refs, (ids_ref, ids_row_ref, trig_scr) = refs[:-3], refs[-3:]
    tokens = cotan_ref.shape[0]
    experts = len(table_refs)
    here = lax.axis_index("expert")
    routes = routes_ref[...]
    gates = gates_ref[...]
    rows = lax.broadcasted_iota(jnp.int32, (experts, tokens), 0)
    expert_ids = (here // 2 * 2 + rows // 2 * 2) % experts + (here + rows) % 2
    first = routes[0:1, :] == expert_ids
    second = routes[1:2, :] == expert_ids
    named = jnp.where(first | second, 1.0, 0.0)
    gate_of = jnp.where(first, gates[0:1, :], 0.0) + jnp.where(second, gates[1:2, :], 0.0)
    earlier = jnp.where(
        lax.broadcasted_iota(jnp.int32, (tokens, tokens), 0)
        < lax.broadcasted_iota(jnp.int32, (tokens, tokens), 1),
        1.0,
        0.0,
    ).astype(jnp.bfloat16)
    ranks = jnp.dot(named.astype(jnp.bfloat16), earlier, preferred_element_type=jnp.float32)
    slot_ids = lax.broadcasted_iota(jnp.int32, (CAP, tokens), 0).astype(jnp.float32)
    cotan = cotan_ref[...]
    for e in range(experts):
        pick = jnp.where((slot_ids == ranks[e : e + 1, :]) & (named[e : e + 1, :] > 0.5), 1.0, 0.0)
        gate_slot = jnp.sum(pick * gate_of[e : e + 1, :], axis=1, keepdims=True)
        picked = jnp.dot(pick.astype(jnp.bfloat16), cotan, preferred_element_type=jnp.float32)
        table_refs[e][...] = (picked * gate_slot).astype(jnp.bfloat16)

    trig_scr[...] = jnp.zeros_like(trig_scr)
    trig_scr[0:1, 0:BLOCKS] = trigger_ref[...].astype(jnp.float32)
    trig = trig_scr[...]
    earlier_b = jnp.where(
        lax.broadcasted_iota(jnp.int32, (LANES, LANES), 0)
        < lax.broadcasted_iota(jnp.int32, (LANES, LANES), 1),
        1.0,
        0.0,
    ).astype(jnp.bfloat16)
    block_ranks = jnp.dot(trig.astype(jnp.bfloat16), earlier_b, preferred_element_type=jnp.float32)
    rank_ids = lax.broadcasted_iota(jnp.int32, (LANES, LANES), 0).astype(jnp.float32)
    match = jnp.where((rank_ids == block_ranks[0:1, :]) & (trig[0:1, :] > 0.5), 1.0, 0.0)
    lane_ids = lax.broadcasted_iota(jnp.int32, (LANES, LANES), 1).astype(jnp.float32)
    column = jnp.sum(match * (lane_ids - 64.0), axis=1, keepdims=True) + 64.0
    ids_ref[...] = jnp.broadcast_to(column[0:TRIG], (TRIG, LANES)).astype(jnp.int32)
    offsets = (lax.broadcasted_iota(jnp.int32, (16, LANES), 1).astype(jnp.float32) - 64.0).astype(jnp.bfloat16)
    row = lax.dot_general(offsets, match.astype(jnp.bfloat16), CONTRACT_LANES, preferred_element_type=jnp.float32)
    ids_row_ref[...] = (row[0:1, :] + 64.0).astype(jnp.int32)


def plan(routes, gates, cotan, trigger, experts):
    return pl.pallas_call(
        plan_kernel,
        out_shape=(
            *[jax.ShapeDtypeStruct((CAP, DW), jnp.bfloat16)] * experts,
            jax.ShapeDtypeStruct((TRIG, LANES), jnp.int32),
            jax.ShapeDtypeStruct((1, LANES), jnp.int32),
        ),
        scratch_shapes=[pltpu.VMEM((8, LANES), jnp.float32)],
        compiler_params=pltpu.CompilerParams(vmem_limit_bytes=PLAN_LIMIT),
        cost_estimate=pl.CostEstimate(flops=200_000_000, bytes_accessed=2_000_000, transcendentals=0),
        name="plan",
    )(routes, gates, cotan, trigger)


def join(left_ref, at, now, prev):
    rows = now.shape[0]
    left_ref[0:rows, at] = now
    left_ref[rows:, at] = prev


def seen_from_here():
    here = lax.axis_index("dp")
    for t in range(SIDE):
        for s in range(SIDE):
            server = (here // SIDE + t) % SIDE * SIDE + (here + s) % SIDE
            at = t * SIDE + s
            yield pl.ds(pl.multiple_of(server * LANES, LANES), LANES), slice(at * LANES, (at + 1) * LANES)


def fetch_kernel(ids_ref, now_hbm, prev_hbm, cotan_ref, right_ref, *refs):
    left_refs, (now_sems, prev_sems) = refs[:-2], refs[-2:]
    rows = cotan_ref.shape[0]
    copies = []
    for j in range(TRIG):
        block = lax.rem(ids_ref[j, 0], 64)
        come = pl.ds(pl.multiple_of(block * BLOCK, BLOCK), BLOCK)
        left_ref, at = left_refs[j // HALF], pl.ds(j % HALF * BLOCK, BLOCK)
        copies.append(pltpu.make_async_copy(now_hbm.at[:, come], left_ref.at[pl.ds(0, rows), at], now_sems.at[j]))
        copies.append(pltpu.make_async_copy(prev_hbm.at[:, come], left_ref.at[pl.ds(rows, rows), at], prev_sems.at[j]))
    for copy in copies:
        copy.start()
    for come, at in seen_from_here():
        right_ref[:, at] = -cotan_ref[:, come]
    for copy in copies:
        copy.wait()


def fetch(ids, now, prev, cotan):
    rows = now.shape[0]
    vmem = pl.BlockSpec(memory_space=pltpu.VMEM)
    hbm = pl.BlockSpec(memory_space=pltpu.HBM)
    left = jax.ShapeDtypeStruct((2 * rows, HALF * BLOCK), now.dtype)
    return pl.pallas_call(
        fetch_kernel,
        out_shape=[jax.ShapeDtypeStruct(cotan.shape, cotan.dtype)] + [left] * (TRIG // HALF),
        in_specs=[pl.BlockSpec(memory_space=pltpu.SMEM), hbm, hbm, vmem],
        out_specs=[vmem] * (1 + TRIG // HALF),
        scratch_shapes=[pltpu.SemaphoreType.DMA((TRIG,)), pltpu.SemaphoreType.DMA((TRIG,))],
        compiler_params=pltpu.CompilerParams(vmem_limit_bytes=FETCH_LIMIT),
        cost_estimate=pl.CostEstimate(flops=100_000_000, bytes_accessed=6_600_000, transcendentals=0),
        name="fetch",
    )(ids, now, prev, cotan)


def arrange_kernel(*refs):
    got_refs, (before_ref, out_ref) = refs[:-2], refs[-2:]
    experts = len(got_refs)
    slots = got_refs[0].shape[0]
    here = lax.axis_index("expert")
    for r, got_ref in enumerate(got_refs):
        source = (here // 2 * 2 + experts - r // 2 * 2) % experts + (here + r) % 2
        rows = pl.ds(pl.multiple_of(source * slots, 8), slots)
        for come, at in seen_from_here():
            out_ref[rows, at] = got_ref[:, come]
    out_ref[experts * slots :, :] = before_ref[...]


def arrange(got, before):
    rows = len(got) * got[0].shape[0] + before.shape[0]
    vmem = pl.BlockSpec(memory_space=pltpu.VMEM)
    return pl.pallas_call(
        arrange_kernel,
        out_shape=jax.ShapeDtypeStruct((rows, before.shape[1]), before.dtype),
        in_specs=[vmem] * (len(got) + 1),
        out_specs=vmem,
        compiler_params=pltpu.CompilerParams(vmem_limit_bytes=FETCH_LIMIT),
        cost_estimate=pl.CostEstimate(flops=100_000_000, bytes_accessed=5_200_000, transcendentals=0),
        name="arrange",
    )(*got, before)


def products_kernel(z_first, row_ref, left_ref, right_ref, *refs):
    own_refs, far_refs = refs[0:SIDE], (None, *refs[SIDE:])
    blocks = left_ref.shape[1]
    row = jnp.broadcast_to(row_ref[...].astype(jnp.float32), (TAIL, LANES)).astype(jnp.bfloat16)
    behind = slice(blocks, blocks + TAIL)
    for k in range(SIDE):
        own_refs[k][0, behind, :] = row
        for m in range(1, SIDE):
            far_refs[m][k, behind, :] = row
    for g in range(0, blocks, GROUP * BLOCK):
        at = slice(g, g + GROUP * BLOCK)
        for t in range(SIDE):
            acc = lax.dot_general(
                left_ref[:, at],
                right_ref[:, t * SIDE * LANES : (t + 1) * SIDE * LANES],
                CONTRACT_ROWS,
                preferred_element_type=jnp.float32,
            )
            for s in range(SIDE):
                piece = acc[:, s * LANES : (s + 1) * LANES].astype(jnp.bfloat16)
                first, second = (t, s) if z_first else (s, t)
                if first == 0:
                    own_refs[second][0, at, :] = piece
                else:
                    far_refs[first][second, at, :] = piece


def products(row, left, right, z_first):
    blocks = left.shape[1]
    vmem = pl.BlockSpec(memory_space=pltpu.VMEM)
    return pl.pallas_call(
        functools.partial(products_kernel, z_first),
        out_shape=[jax.ShapeDtypeStruct((1, blocks + TAIL, LANES), jnp.bfloat16)] * SIDE
        + [jax.ShapeDtypeStruct((SIDE, blocks + TAIL, LANES), jnp.bfloat16)] * (SIDE - 1),
        in_specs=[vmem] * 3,
        out_specs=[vmem] * (2 * SIDE - 1),
        compiler_params=pltpu.CompilerParams(vmem_limit_bytes=PRODUCTS_LIMIT),
        cost_estimate=pl.CostEstimate(
            flops=2 * left.shape[0] * blocks * DW, bytes_accessed=8_000_000, transcendentals=0
        ),
        name="products",
    )(row, left, right)


def norms_kernel(now_ref, prev_ref, right_ref, out_ref, left_ref):
    join(left_ref, slice(None), now_ref[...], prev_ref[...])
    totals = [jnp.zeros((1, LANES), jnp.float32)] * GROUP
    for n in range(DW // WIDE):
        acc = lax.dot_general(
            left_ref[...],
            right_ref[:, n * WIDE : (n + 1) * WIDE],
            CONTRACT_ROWS,
            preferred_element_type=jnp.float32,
        )
        for j in range(GROUP):
            part = acc[j * BLOCK : (j + 1) * BLOCK, :]
            sums = jnp.sum(part * part, axis=0, keepdims=True)
            for s in range(WIDE // LANES):
                totals[j] = totals[j] + sums[:, s * LANES : (s + 1) * LANES]
    for j in range(GROUP):
        out_ref[j] = totals[j]


def norms(now, prev, right):
    rows = now.shape[0]
    return pl.pallas_call(
        norms_kernel,
        out_shape=jax.ShapeDtypeStruct((BLOCKS, 1, LANES), jnp.float32),
        grid=(BLOCKS // GROUP,),
        in_specs=[
            pl.BlockSpec((rows, GROUP * BLOCK), lambda b: (0, b)),
            pl.BlockSpec((rows, GROUP * BLOCK), lambda b: (0, b)),
            pl.BlockSpec((2 * rows, DW), lambda b: (0, 0)),
        ],
        out_specs=pl.BlockSpec((GROUP, 1, LANES), lambda b: (b, 0, 0)),
        scratch_shapes=[
            pltpu.VMEM((2 * rows, GROUP * BLOCK), jnp.bfloat16),
        ],
        compiler_params=pltpu.CompilerParams(dimension_semantics=("arbitrary",), vmem_limit_bytes=LIMIT),
        cost_estimate=pl.CostEstimate(
            flops=4 * rows * FFW * DW, bytes_accessed=4 * rows * FFW + 2_600_000, transcendentals=0
        ),
        name="norms",
    )(now, prev, right)


def update_kernel(pieces, last, base_ref, *refs):
    got_refs, (out_ref, *rest) = refs[: len(pieces)], refs[len(pieces) :]
    ids_scr, ids_ref, ids_sem = rest[-3:]
    row = 0
    for got_ref, (parts, _) in zip(got_refs, pieces):
        for k in range(parts):
            tail = got_ref[k, got_ref.shape[1] - TAIL :, :].astype(jnp.float32)
            ids_scr[row : row + 1, :] = tail[0:1, :].astype(jnp.int32)
            row += 1
    copy = pltpu.make_async_copy(ids_scr, ids_ref, ids_sem)
    copy.start()
    out_ref[...] = base_ref[...]
    copy.wait()
    row = 0
    for got_ref, (parts, start) in zip(got_refs, pieces):
        count = got_ref.shape[1] // BLOCK
        for k in range(parts):

            def add(j, carry, got_ref=got_ref, k=k, row=row, start=start):
                block = ids_ref[row, start + j]

                @pl.when(block < 64)
                def _():
                    at = pl.ds(pl.multiple_of(block * BLOCK, BLOCK), BLOCK)
                    come = pl.ds(pl.multiple_of(j * BLOCK, BLOCK), BLOCK)
                    out_ref[at, :] += got_ref[k, come, :].astype(jnp.float32)

                return carry

            lax.fori_loop(0, count, add, 0)
            row += 1
    if last:
        squares_ref, scr = rest[0], rest[1]
        scr[...] = jnp.zeros_like(scr)
        for b in range(BLOCKS):
            x = out_ref[b * BLOCK : (b + 1) * BLOCK, :]
            scr[b : b + 1, :] = jnp.sum(x * x, axis=0, keepdims=True)
        squares_ref[...] = lax.dot_general(
            jnp.ones((16, LANES), jnp.float32),
            scr[...],
            CONTRACT_LANES,
            precision=lax.Precision.HIGHEST,
            preferred_element_type=jnp.float32,
        )


def update(base, got, pieces, last):
    vmem = pl.BlockSpec(memory_space=pltpu.VMEM)
    out_shape = [jax.ShapeDtypeStruct(base.shape, jnp.float32)]
    scratch = []
    if last:
        out_shape.append(jax.ShapeDtypeStruct((16, LANES), jnp.float32))
        scratch.append(pltpu.VMEM((LANES, LANES), jnp.float32))
    rows = -(-sum(parts for parts, _ in pieces) // 8) * 8
    return pl.pallas_call(
        functools.partial(update_kernel, pieces, last),
        out_shape=out_shape,
        in_specs=[vmem] * (1 + len(got)),
        out_specs=[vmem] * len(out_shape),
        scratch_shapes=[
            *scratch,
            pltpu.VMEM((rows, LANES), jnp.int32),
            pltpu.SMEM((rows, LANES), jnp.int32),
            pltpu.SemaphoreType.DMA,
        ],
        compiler_params=pltpu.CompilerParams(vmem_limit_bytes=UPDATE_LIMIT),
        cost_estimate=pl.CostEstimate(flops=5_000_000_000, bytes_accessed=16_000_000, transcendentals=0),
        name="update_last" if last else "update",
    )(base, *got)


def cross(experts, r):
    return [(e, (e // 2 * 2 + r // 2 * 2) % experts + (e + r) % 2) for e in range(experts)]


def shift(workers, dz, dy):
    side = SIDE
    return [
        (z * side + y, ((z + dz) % side) * side + (y + dy) % side) for z in range(workers // side) for y in range(side)
    ]


def local(cotangents, routes, gate_probs, hidden_now, hidden_prev, cotan_prev, trigger, stale_sum):
    experts = lax.axis_size("expert")
    workers = lax.axis_size("dp")
    columns = DW // workers
    *tables, ids, ids_row = plan(routes.T, gate_probs.T, cotangents, trigger.reshape(1, BLOCKS), experts)
    exchange = functools.partial(lax.all_to_all, split_axis=0, concat_axis=0, tiled=True)
    arrived = [tables[0]] + [None] * (experts - 1)
    for r in HOPS:
        arrived[r] = lax.ppermute(tables[r], "expert", cross(experts, r))
    now = hidden_now.reshape(-1, FFW)
    prev = hidden_prev.reshape(-1, FFW)
    before, left_a, left_b = fetch(ids, now, prev, cotan_prev.reshape(-1, DW))
    right = arrange(arrived, before)

    def along_y(x, k):
        return lax.ppermute(x, "dp", shift(workers, 0, k))

    def along_z(x, k):
        return lax.ppermute(x, "dp", shift(workers, k, 0))

    def stage_one(left, z_first, near, far):
        sent = products(ids_row, left, right, z_first)
        own, relay = {0: sent[0]}, {}
        for k in ORDER:
            relay[k] = near(sent[SIDE - 1 + k], k)
        for k in ORDER:
            own[k] = far(sent[k], k)
        return own, relay

    def stage_two(relay, far):
        got = {}
        for k in ORDER:
            got[k] = far(jnp.stack([relay[j][k] for j in range(1, SIDE)]), k)
        return got

    own_a, relay_a = stage_one(left_a, False, along_y, along_z)
    own_b, relay_b = stage_one(left_b, True, along_z, along_y)
    squared = norms(now, prev, right)
    relay_a, squared = lax.optimization_barrier((relay_a, squared))
    second_a = stage_two(relay_a, along_z)
    second_b = stage_two(relay_b, along_y)
    diff_norms = jnp.sum(squared, axis=(1, 2)) / (BLOCK * DW)
    near_a = [own_a[k] for k in range(SIDE)] + [relay_a[k] for k in ORDER]
    near_b = [own_b[k] for k in range(SIDE)] + [relay_b[k] for k in ORDER]
    (current,) = update(
        stale_sum.reshape(FFW, columns),
        near_a + near_b,
        [(1, 0)] * len(near_a) + [(1, HALF)] * len(near_b),
        False,
    )
    (current,) = update(
        current,
        [second_a[k] for k in ORDER[:2]] + [second_b[k] for k in ORDER[:2]],
        [(SIDE - 1, 0)] * 2 + [(SIDE - 1, HALF)] * 2,
        False,
    )
    current, squares = update(
        current, [second_a[ORDER[2]], second_b[ORDER[2]]], [(SIDE - 1, 0), (SIDE - 1, HALF)], True
    )
    everyone = exchange(squares.reshape(workers, 1, LANES), "dp").reshape(workers, LANES)
    norm_totals = jnp.sum(everyone, axis=0)[:BLOCKS] / (BLOCK * DW)
    margins = diff_norms - trigger_weight * norm_totals
    return (current.reshape(1, FFW, columns), margins.reshape(1, 1, BLOCKS))


def solution(mesh):
    return jax.shard_map(
        local,
        mesh=mesh,
        in_specs=(
            P(("expert", "dp"), None),
            P(("expert", "dp"), None),
            P(("expert", "dp"), None),
            P("expert", "dp", None, None, None),
            P("expert", "dp", None, None, None),
            P("expert", "dp", None, None),
            P("expert", "dp", None),
            P("expert", None, "dp"),
        ),
        out_specs=(P("expert", None, "dp"), P("expert", "dp", None)),
        check_vma=False,
    )
```

```python
import functools

import jax
import jax.numpy as jnp
from jax import lax
from jax.experimental import pallas as pl
from jax.experimental.pallas import tpu as pltpu
from jax.sharding import PartitionSpec as P


DW = 2048
FFW = 7168
BLOCK = 128
BLOCKS = 56
TRIG = 16
CAP = 40
LANES = 128
GROUP = 4
WIDE = 512
SIDE = 4
TAIL = 16
HALF = 8
ORDER = (1, 3, 2)
HOPS = (4, 5, 2, 6, 3, 7, 1)
PLAN_LIMIT = 58 * 1024 * 1024
FETCH_LIMIT = 16 * 1024 * 1024
PRODUCTS_LIMIT = 16 * 1024 * 1024
LIMIT = 20 * 1024 * 1024
UPDATE_LIMIT = 20 * 1024 * 1024


trigger_weight = 0.1

CONTRACT_ROWS = (((0,), (0,)), ((), ()))
CONTRACT_LANES = (((1,), (1,)), ((), ()))


def plan_kernel(routes_ref, gates_ref, cotan_ref, trigger_ref, *refs):
    table_refs, (ids_ref, ids_row_ref, trig_scr) = refs[:-3], refs[-3:]
    tokens = cotan_ref.shape[0]
    experts = len(table_refs)
    here = lax.axis_index("expert")
    routes = routes_ref[...]
    gates = gates_ref[...]
    rows = lax.broadcasted_iota(jnp.int32, (experts, tokens), 0)
    expert_ids = (here // 2 * 2 + rows // 2 * 2) % experts + (here + rows) % 2
    first = routes[0:1, :] == expert_ids
    second = routes[1:2, :] == expert_ids
    named = jnp.where(first | second, 1.0, 0.0)
    gate_of = jnp.where(first, gates[0:1, :], 0.0) + jnp.where(second, gates[1:2, :], 0.0)
    earlier = jnp.where(
        lax.broadcasted_iota(jnp.int32, (tokens, tokens), 0)
        < lax.broadcasted_iota(jnp.int32, (tokens, tokens), 1),
        1.0,
        0.0,
    ).astype(jnp.bfloat16)
    ranks = jnp.dot(named.astype(jnp.bfloat16), earlier, preferred_element_type=jnp.float32)
    slot_ids = lax.broadcasted_iota(jnp.int32, (CAP, tokens), 0).astype(jnp.float32)
    cotan = cotan_ref[...]
    for e in range(experts):
        pick = jnp.where((slot_ids == ranks[e : e + 1, :]) & (named[e : e + 1, :] > 0.5), 1.0, 0.0)
        gate_slot = jnp.sum(pick * gate_of[e : e + 1, :], axis=1, keepdims=True)
        picked = jnp.dot(pick.astype(jnp.bfloat16), cotan, preferred_element_type=jnp.float32)
        table_refs[e][...] = (picked * gate_slot).astype(jnp.bfloat16)

    trig_scr[...] = jnp.zeros_like(trig_scr)
    trig_scr[0:1, 0:BLOCKS] = trigger_ref[...].astype(jnp.float32)
    trig = trig_scr[...]
    earlier_b = jnp.where(
        lax.broadcasted_iota(jnp.int32, (LANES, LANES), 0)
        < lax.broadcasted_iota(jnp.int32, (LANES, LANES), 1),
        1.0,
        0.0,
    ).astype(jnp.bfloat16)
    block_ranks = jnp.dot(trig.astype(jnp.bfloat16), earlier_b, preferred_element_type=jnp.float32)
    rank_ids = lax.broadcasted_iota(jnp.int32, (LANES, LANES), 0).astype(jnp.float32)
    match = jnp.where((rank_ids == block_ranks[0:1, :]) & (trig[0:1, :] > 0.5), 1.0, 0.0)
    lane_ids = lax.broadcasted_iota(jnp.int32, (LANES, LANES), 1).astype(jnp.float32)
    column = jnp.sum(match * (lane_ids - 64.0), axis=1, keepdims=True) + 64.0
    ids_ref[...] = jnp.broadcast_to(column[0:TRIG], (TRIG, LANES)).astype(jnp.int32)
    offsets = (lax.broadcasted_iota(jnp.int32, (16, LANES), 1).astype(jnp.float32) - 64.0).astype(jnp.bfloat16)
    row = lax.dot_general(offsets, match.astype(jnp.bfloat16), CONTRACT_LANES, preferred_element_type=jnp.float32)
    ids_row_ref[...] = (row[0:1, :] + 64.0).astype(jnp.int32)


def plan(routes, gates, cotan, trigger, experts):
    return pl.pallas_call(
        plan_kernel,
        out_shape=(
            *[jax.ShapeDtypeStruct((CAP, DW), jnp.bfloat16)] * experts,
            jax.ShapeDtypeStruct((TRIG, LANES), jnp.int32),
            jax.ShapeDtypeStruct((1, LANES), jnp.int32),
        ),
        scratch_shapes=[pltpu.VMEM((8, LANES), jnp.float32)],
        compiler_params=pltpu.CompilerParams(vmem_limit_bytes=PLAN_LIMIT),
        cost_estimate=pl.CostEstimate(flops=200_000_000, bytes_accessed=2_000_000, transcendentals=0),
        name="plan",
    )(routes, gates, cotan, trigger)


def join(left_ref, at, now, prev):
    rows = now.shape[0]
    left_ref[0:rows, at] = now
    left_ref[rows:, at] = prev


def seen_from_here():
    here = lax.axis_index("dp")
    for t in range(SIDE):
        for s in range(SIDE):
            server = (here // SIDE + t) % SIDE * SIDE + (here + s) % SIDE
            at = t * SIDE + s
            yield pl.ds(pl.multiple_of(server * LANES, LANES), LANES), slice(at * LANES, (at + 1) * LANES)


def fetch_kernel(ids_ref, now_hbm, prev_hbm, cotan_ref, right_ref, *refs):
    left_refs, (now_sems, prev_sems) = refs[:-2], refs[-2:]
    rows = cotan_ref.shape[0]
    copies = []
    for j in range(TRIG):
        block = lax.rem(ids_ref[j, 0], 64)
        come = pl.ds(pl.multiple_of(block * BLOCK, BLOCK), BLOCK)
        left_ref, at = left_refs[j // HALF], pl.ds(j % HALF * BLOCK, BLOCK)
        copies.append(pltpu.make_async_copy(now_hbm.at[:, come], left_ref.at[pl.ds(0, rows), at], now_sems.at[j]))
        copies.append(pltpu.make_async_copy(prev_hbm.at[:, come], left_ref.at[pl.ds(rows, rows), at], prev_sems.at[j]))
    for copy in copies:
        copy.start()
    for come, at in seen_from_here():
        right_ref[:, at] = -cotan_ref[:, come]
    for copy in copies:
        copy.wait()


def fetch(ids, now, prev, cotan):
    rows = now.shape[0]
    vmem = pl.BlockSpec(memory_space=pltpu.VMEM)
    hbm = pl.BlockSpec(memory_space=pltpu.HBM)
    left = jax.ShapeDtypeStruct((2 * rows, HALF * BLOCK), now.dtype)
    return pl.pallas_call(
        fetch_kernel,
        out_shape=[jax.ShapeDtypeStruct(cotan.shape, cotan.dtype)] + [left] * (TRIG // HALF),
        in_specs=[pl.BlockSpec(memory_space=pltpu.SMEM), hbm, hbm, vmem],
        out_specs=[vmem] * (1 + TRIG // HALF),
        scratch_shapes=[pltpu.SemaphoreType.DMA((TRIG,)), pltpu.SemaphoreType.DMA((TRIG,))],
        compiler_params=pltpu.CompilerParams(vmem_limit_bytes=FETCH_LIMIT),
        cost_estimate=pl.CostEstimate(flops=100_000_000, bytes_accessed=6_600_000, transcendentals=0),
        name="fetch",
    )(ids, now, prev, cotan)


def arrange_kernel(*refs):
    got_refs, (before_ref, out_ref) = refs[:-2], refs[-2:]
    experts = len(got_refs)
    slots = got_refs[0].shape[0]
    here = lax.axis_index("expert")
    for r, got_ref in enumerate(got_refs):
        source = (here // 2 * 2 + experts - r // 2 * 2) % experts + (here + r) % 2
        rows = pl.ds(pl.multiple_of(source * slots, 8), slots)
        for come, at in seen_from_here():
            out_ref[rows, at] = got_ref[:, come]
    out_ref[experts * slots :, :] = before_ref[...]


def arrange(got, before):
    rows = len(got) * got[0].shape[0] + before.shape[0]
    vmem = pl.BlockSpec(memory_space=pltpu.VMEM)
    return pl.pallas_call(
        arrange_kernel,
        out_shape=jax.ShapeDtypeStruct((rows, before.shape[1]), before.dtype),
        in_specs=[vmem] * (len(got) + 1),
        out_specs=vmem,
        compiler_params=pltpu.CompilerParams(vmem_limit_bytes=FETCH_LIMIT),
        cost_estimate=pl.CostEstimate(flops=100_000_000, bytes_accessed=5_200_000, transcendentals=0),
        name="arrange",
    )(*got, before)


def products_kernel(z_first, row_ref, left_ref, right_ref, *refs):
    own_refs, far_refs = refs[0:SIDE], (None, *refs[SIDE:])
    blocks = left_ref.shape[1]
    row = jnp.broadcast_to(row_ref[...].astype(jnp.float32), (TAIL, LANES)).astype(jnp.bfloat16)
    behind = slice(blocks, blocks + TAIL)
    for k in range(SIDE):
        own_refs[k][0, behind, :] = row
        for m in range(1, SIDE):
            far_refs[m][k, behind, :] = row
    for g in range(0, blocks, GROUP * BLOCK):
        at = slice(g, g + GROUP * BLOCK)
        for t in range(SIDE):
            acc = lax.dot_general(
                left_ref[:, at],
                right_ref[:, t * SIDE * LANES : (t + 1) * SIDE * LANES],
                CONTRACT_ROWS,
                preferred_element_type=jnp.float32,
            )
            for s in range(SIDE):
                piece = acc[:, s * LANES : (s + 1) * LANES].astype(jnp.bfloat16)
                first, second = (t, s) if z_first else (s, t)
                if first == 0:
                    own_refs[second][0, at, :] = piece
                else:
                    far_refs[first][second, at, :] = piece


def products(row, left, right, z_first):
    blocks = left.shape[1]
    vmem = pl.BlockSpec(memory_space=pltpu.VMEM)
    return pl.pallas_call(
        functools.partial(products_kernel, z_first),
        out_shape=[jax.ShapeDtypeStruct((1, blocks + TAIL, LANES), jnp.bfloat16)] * SIDE
        + [jax.ShapeDtypeStruct((SIDE, blocks + TAIL, LANES), jnp.bfloat16)] * (SIDE - 1),
        in_specs=[vmem] * 3,
        out_specs=[vmem] * (2 * SIDE - 1),
        compiler_params=pltpu.CompilerParams(vmem_limit_bytes=PRODUCTS_LIMIT),
        cost_estimate=pl.CostEstimate(
            flops=2 * left.shape[0] * blocks * DW, bytes_accessed=8_000_000, transcendentals=0
        ),
        name="products",
    )(row, left, right)


def norms_kernel(now_ref, prev_ref, right_ref, out_ref, left_ref):
    join(left_ref, slice(None), now_ref[...], prev_ref[...])
    totals = [jnp.zeros((1, LANES), jnp.float32)] * GROUP
    for n in range(DW // WIDE):
        acc = lax.dot_general(
            left_ref[...],
            right_ref[:, n * WIDE : (n + 1) * WIDE],
            CONTRACT_ROWS,
            preferred_element_type=jnp.float32,
        )
        for j in range(GROUP):
            part = acc[j * BLOCK : (j + 1) * BLOCK, :]
            sums = jnp.sum(part * part, axis=0, keepdims=True)
            for s in range(WIDE // LANES):
                totals[j] = totals[j] + sums[:, s * LANES : (s + 1) * LANES]
    for j in range(GROUP):
        out_ref[j] = totals[j]


def norms(now, prev, right):
    rows = now.shape[0]
    return pl.pallas_call(
        norms_kernel,
        out_shape=jax.ShapeDtypeStruct((BLOCKS, 1, LANES), jnp.float32),
        grid=(BLOCKS // GROUP,),
        in_specs=[
            pl.BlockSpec((rows, GROUP * BLOCK), lambda b: (0, b)),
            pl.BlockSpec((rows, GROUP * BLOCK), lambda b: (0, b)),
            pl.BlockSpec((2 * rows, DW), lambda b: (0, 0)),
        ],
        out_specs=pl.BlockSpec((GROUP, 1, LANES), lambda b: (b, 0, 0)),
        scratch_shapes=[
            pltpu.VMEM((2 * rows, GROUP * BLOCK), jnp.bfloat16),
        ],
        compiler_params=pltpu.CompilerParams(dimension_semantics=("arbitrary",), vmem_limit_bytes=LIMIT),
        cost_estimate=pl.CostEstimate(
            flops=4 * rows * FFW * DW, bytes_accessed=4 * rows * FFW + 2_600_000, transcendentals=0
        ),
        name="norms",
    )(now, prev, right)


def update_kernel(pieces, last, base_ref, *refs):
    got_refs, (out_ref, *rest) = refs[: len(pieces)], refs[len(pieces) :]
    ids_scr, ids_ref, ids_sem = rest[-3:]
    if last:
        result_hbm, (squares_ref, scr, out_ref, result_sem) = out_ref, rest[:4]
    row = 0
    for got_ref, (parts, _) in zip(got_refs, pieces):
        for k in range(parts):
            tail = got_ref[k, got_ref.shape[1] - TAIL :, :].astype(jnp.float32)
            ids_scr[row : row + 1, :] = tail[0:1, :].astype(jnp.int32)
            row += 1
    copy = pltpu.make_async_copy(ids_scr, ids_ref, ids_sem)
    copy.start()
    out_ref[...] = base_ref[...]
    copy.wait()
    row = 0
    for got_ref, (parts, start) in zip(got_refs, pieces):
        count = got_ref.shape[1] // BLOCK
        for k in range(parts):

            def add(j, carry, got_ref=got_ref, k=k, row=row, start=start):
                block = ids_ref[row, start + j]

                @pl.when(block < 64)
                def _():
                    at = pl.ds(pl.multiple_of(block * BLOCK, BLOCK), BLOCK)
                    come = pl.ds(pl.multiple_of(j * BLOCK, BLOCK), BLOCK)
                    out_ref[at, :] += got_ref[k, come, :].astype(jnp.float32)

                return carry

            lax.fori_loop(0, count, add, 0)
            row += 1
    if last:
        result = pltpu.make_async_copy(out_ref, result_hbm, result_sem)
        result.start()
        scr[...] = jnp.zeros_like(scr)
        for b in range(BLOCKS):
            x = out_ref[b * BLOCK : (b + 1) * BLOCK, :]
            scr[b : b + 1, :] = jnp.sum(x * x, axis=0, keepdims=True)
        squares_ref[...] = lax.dot_general(
            jnp.ones((16, LANES), jnp.float32),
            scr[...],
            CONTRACT_LANES,
            precision=lax.Precision.HIGHEST,
            preferred_element_type=jnp.float32,
        )
        result.wait()


def update(base, got, pieces, last):
    vmem = pl.BlockSpec(memory_space=pltpu.VMEM)
    out_shape = [jax.ShapeDtypeStruct(base.shape, jnp.float32)]
    scratch = []
    if last:
        out_shape.append(jax.ShapeDtypeStruct((16, LANES), jnp.float32))
        scratch += [pltpu.VMEM((LANES, LANES), jnp.float32), pltpu.VMEM(base.shape, jnp.float32)]
        scratch.append(pltpu.SemaphoreType.DMA)
    rows = -(-sum(parts for parts, _ in pieces) // 8) * 8
    return pl.pallas_call(
        functools.partial(update_kernel, pieces, last),
        out_shape=out_shape,
        in_specs=[vmem] * (1 + len(got)),
        out_specs=[pl.BlockSpec(memory_space=pltpu.HBM), vmem] if last else [vmem],
        scratch_shapes=[
            *scratch,
            pltpu.VMEM((rows, LANES), jnp.int32),
            pltpu.SMEM((rows, LANES), jnp.int32),
            pltpu.SemaphoreType.DMA,
        ],
        compiler_params=pltpu.CompilerParams(vmem_limit_bytes=UPDATE_LIMIT),
        cost_estimate=pl.CostEstimate(flops=5_000_000_000, bytes_accessed=16_000_000, transcendentals=0),
        name="update_last" if last else "update",
    )(base, *got)


def cross(experts, r):
    return [(e, (e // 2 * 2 + r // 2 * 2) % experts + (e + r) % 2) for e in range(experts)]


def shift(workers, dz, dy):
    side = SIDE
    return [
        (z * side + y, ((z + dz) % side) * side + (y + dy) % side) for z in range(workers // side) for y in range(side)
    ]


def local(cotangents, routes, gate_probs, hidden_now, hidden_prev, cotan_prev, trigger, stale_sum):
    experts = lax.axis_size("expert")
    workers = lax.axis_size("dp")
    columns = DW // workers
    *tables, ids, ids_row = plan(routes.T, gate_probs.T, cotangents, trigger.reshape(1, BLOCKS), experts)
    exchange = functools.partial(lax.all_to_all, split_axis=0, concat_axis=0, tiled=True)
    arrived = [tables[0]] + [None] * (experts - 1)
    for r in HOPS:
        arrived[r] = lax.ppermute(tables[r], "expert", cross(experts, r))
    now = hidden_now.reshape(-1, FFW)
    prev = hidden_prev.reshape(-1, FFW)
    before, left_a, left_b = fetch(ids, now, prev, cotan_prev.reshape(-1, DW))
    right = arrange(arrived, before)

    def along_y(x, k):
        return lax.ppermute(x, "dp", shift(workers, 0, k))

    def along_z(x, k):
        return lax.ppermute(x, "dp", shift(workers, k, 0))

    def stage_one(left, z_first, near, far):
        sent = products(ids_row, left, right, z_first)
        own, relay = {0: sent[0]}, {}
        for k in ORDER:
            relay[k] = near(sent[SIDE - 1 + k], k)
        for k in ORDER:
            own[k] = far(sent[k], k)
        return own, relay

    def stage_two(relay, far):
        got = {}
        for k in ORDER:
            got[k] = far(jnp.stack([relay[j][k] for j in range(1, SIDE)]), k)
        return got

    own_a, relay_a = stage_one(left_a, False, along_y, along_z)
    own_b, relay_b = stage_one(left_b, True, along_z, along_y)
    squared = norms(now, prev, right)
    relay_a, squared = lax.optimization_barrier((relay_a, squared))
    second_a = stage_two(relay_a, along_z)
    second_b = stage_two(relay_b, along_y)
    diff_norms = jnp.sum(squared, axis=(1, 2)) / (BLOCK * DW)
    near_a = [own_a[k] for k in range(SIDE)] + [relay_a[k] for k in ORDER]
    near_b = [own_b[k] for k in range(SIDE)] + [relay_b[k] for k in ORDER]
    (current,) = update(
        stale_sum.reshape(FFW, columns),
        near_a + near_b,
        [(1, 0)] * len(near_a) + [(1, HALF)] * len(near_b),
        False,
    )
    (current,) = update(
        current,
        [second_a[k] for k in ORDER[:2]] + [second_b[k] for k in ORDER[:2]],
        [(SIDE - 1, 0)] * 2 + [(SIDE - 1, HALF)] * 2,
        False,
    )
    current, squares = update(
        current, [second_a[ORDER[2]], second_b[ORDER[2]]], [(SIDE - 1, 0), (SIDE - 1, HALF)], True
    )
    everyone = exchange(squares.reshape(workers, 1, LANES), "dp").reshape(workers, LANES)
    norm_totals = jnp.sum(everyone, axis=0)[:BLOCKS] / (BLOCK * DW)
    margins = diff_norms - trigger_weight * norm_totals
    return (current.reshape(1, FFW, columns), margins.reshape(1, 1, BLOCKS))


def solution(mesh):
    return jax.shard_map(
        local,
        mesh=mesh,
        in_specs=(
            P(("expert", "dp"), None),
            P(("expert", "dp"), None),
            P(("expert", "dp"), None),
            P("expert", "dp", None, None, None),
            P("expert", "dp", None, None, None),
            P("expert", "dp", None, None),
            P("expert", "dp", None),
            P("expert", None, "dp"),
        ),
        out_specs=(P("expert", None, "dp"), P("expert", "dp", None)),
        check_vma=False,
    )
```
